256 devices in a mesh: dp: 16 (over z_lo, y, core), mp: 16 (over z_hi, x).
Axes of the slice: x: 4, y: 4, z: 8 (z_hi: 4, z_lo: 2; z = z_hi * 2 + z_lo), core: 2. Of those that a mesh axis runs over, the one named last changes fastest.
Arguments:
- tokens: bfloat16 [4096, 1024], P('dp'), may hold values from -6 to 6
- lengths: int32 [16], P('dp'), may hold values from 64 to 256
- cotangent: bfloat16 [4096, 1024], P('dp'), may hold values from -6 to 6
- triple_weight: bfloat16 [2, 1024, 3, 1024], P(None, None, None, 'mp'), may hold values from -0.1875 to 0.1875
- output_weight: bfloat16 [2, 1024, 1024], P(None, None, 'mp'), may hold values from -0.1875 to 0.1875
- upward_weight: bfloat16 [2, 1024, 4096], P(None, None, 'mp'), may hold values from -0.1875 to 0.1875
- downward_weight: bfloat16 [2, 1024, 4096], P(None, None, 'mp'), may hold values from -0.09375 to 0.09375
Outputs:
- final_stream: bfloat16 [4096, 1024], P('dp')
- triple_grad: float32 [2, 1024, 3, 1024], P(None, 'dp', None, 'mp')
- output_grad: float32 [2, 1024, 1024], P(None, 'dp', 'mp')
- upward_grad: float32 [2, 1024, 4096], P(None, 'dp', 'mp')
- downward_grad: float32 [2, 1024, 4096], P(None, 'dp', 'mp')
The draws below stay inside these ranges and needn't reach their ends.
Inputs may be any that keep to these rules, and one draw needn't show every extreme that they name: lengths[s] counts the live candidates of slate s; its other positions are padding.
All inputs are finite; a program needn't handle non-finite values.
Results may differ from the reference program's by a relative error of at most 0.04.
Values may be sent and summed in bfloat16 or wider, within the bound.
No kernel may reach another device: no remote copies, remote signals or barrier semaphores. Data moves between devices by JAX's collectives and lax.ppermute only.
A program may use at most 64 MiB of HBM per device.

```python
import jax
import jax.numpy as jnp
from jax import lax

D = 1024
HEADS = 16
FF = 4096
HD = 64
SLATE = 256
LAYERS = 2
TOKENS = 4096
SLATES = 16
N_MP = 16


def place_ends(values, key, smallest, high):
    spot = [jax.random.randint(jax.random.fold_in(key, axis), (), 0, length) for axis, length in enumerate(values.shape)]
    widest = values.shape.index(max(values.shape))
    next_to = spot[:widest] + [(spot[widest] + 1) % values.shape[widest]] + spot[widest + 1:]
    return values.at[tuple(spot)].set(smallest).at[tuple(next_to)].set(high)


def levels(own_key, dims, shards, low, top_value):
    def one(dim, parts):
        draws = jax.random.uniform(jax.random.fold_in(jax.random.fold_in(own_key, 6), dim), (parts,), jnp.float32, low / len(shards), top_value / len(shards))
        return jnp.repeat(jnp.exp(draws), dims[dim] // parts).reshape((-1,) + (1,) * (len(dims) - dim - 1))

    gain = one(*shards[0])
    for cut in shards[1:]:
        gain = gain * one(*cut)
    return gain


def noise(key, shape, width, reach, pieces=(), held_as=jnp.bfloat16):
    drawn = jax.random.normal(key, shape, jnp.float32) * width
    if len(pieces) > 0:
        drawn = levels(key, shape, pieces, -0.22, 0.18) * drawn
    return jnp.clip(drawn, min=-reach, max=reach).astype(held_as)


def setup_inputs(seed: int = 0) -> dict:
    keys = jax.random.split(jax.random.key(seed), 8)
    tokens = noise(keys[0], (TOKENS, D), 1.0, 6.0, ((0, 16),))
    lengths = place_ends(jax.random.randint(keys[1], (SLATES,), SLATE // 4, SLATE + 1), jax.random.fold_in(keys[1], 1), SLATE // 4, SLATE).astype(jnp.int32)
    cotangent = noise(keys[2], (TOKENS, D), 1.0, 6.0, ((0, 16),))
    triple_weight = noise(keys[3], (LAYERS, D, 3, D), D ** -0.5, 0.1875, ((3, 16),))
    output_weight = noise(keys[4], (LAYERS, D, D), D ** -0.5, 0.1875, ((2, 16),))
    upward_weight = noise(keys[5], (LAYERS, D, FF), D ** -0.5, 0.1875, ((2, 16),))
    downward_weight = noise(keys[6], (LAYERS, D, FF), FF ** -0.5, 0.09375, ((2, 16),))
    return dict(tokens=tokens, lengths=lengths, cotangent=cotangent, triple_weight=triple_weight, output_weight=output_weight, upward_weight=upward_weight, downward_weight=downward_weight)


epsilon = 1e-06

def normalize(stream):
    widened = stream.astype(jnp.float32)
    rscale = lax.rsqrt(lax.optimization_barrier(jnp.mean(widened * widened, axis=-1, keepdims=True)) + epsilon)
    scaled = widened * rscale
    return (scaled.astype(jnp.bfloat16), scaled, rscale)

def norm_backward(scaled, rscale, upward):
    inner = lax.optimization_barrier(jnp.mean(upward * scaled, axis=-1, keepdims=True))
    return rscale * (upward - scaled * inner)

def smooth_gate(preact):
    return jax.nn.gelu(preact, approximate=True)

def attend(queries, key_rows, values, lengths):
    live_keys = (jnp.arange(SLATE)[None, :] < lengths[:, None]).astype(jnp.float32)
    scores = jnp.einsum('bqhe,bkhe->bhqk', queries.astype(jnp.float32), key_rows.astype(jnp.float32)) * HD ** (-0.5)
    weights = jnp.exp(scores) * live_keys[:, None, None, :]
    probs = weights / lax.optimization_barrier(jnp.sum(weights, axis=-1, keepdims=True))
    probs_low = probs.astype(jnp.bfloat16)
    context = jnp.einsum('bhqk,bkhe->bqhe', probs_low.astype(jnp.float32), values.astype(jnp.float32)).astype(jnp.bfloat16)
    return (probs, probs_low, context)

def attend_backward(probs, probs_low, queries, key_rows, values, grad_context):
    grad_prob = jnp.einsum('bqhe,bkhe->bhqk', grad_context.astype(jnp.float32), values.astype(jnp.float32))
    grad_value = jnp.einsum('bhqk,bqhe->bkhe', probs_low.astype(jnp.float32), grad_context.astype(jnp.float32)).astype(jnp.bfloat16)
    inner = lax.optimization_barrier(jnp.sum(grad_prob * probs, axis=-1, keepdims=True))
    grad_score = (probs * (grad_prob - inner) * HD ** (-0.5)).astype(jnp.bfloat16)
    grad_query = jnp.einsum('bhqk,bkhe->bqhe', grad_score.astype(jnp.float32), key_rows.astype(jnp.float32)).astype(jnp.bfloat16)
    grad_key = jnp.einsum('bhqk,bqhe->bkhe', grad_score.astype(jnp.float32), queries.astype(jnp.float32)).astype(jnp.bfloat16)
    return (grad_query, grad_key, grad_value)

def contract_rows(left, right):
    return lax.dot_general(left, right, (((0,), (0,)), ((), ())), preferred_element_type=jnp.float32)

def split_groups(matrix):
    return jnp.moveaxis(matrix.reshape(matrix.shape[0], N_MP, -1), 1, 0)

def split_triples(matrix):
    leading = matrix.shape[0]
    return matrix.reshape(leading, 3, N_MP, -1).transpose(2, 0, 1, 3).reshape(N_MP, leading, -1)

def group_total(left_parts, right_parts):

    def add_group(running, operands):
        addend = lax.dot_general(operands[0], operands[1], (((1,), (1,)), ((), ())), preferred_element_type=jnp.float32)
        return (running + lax.optimization_barrier(addend.astype(jnp.bfloat16)).astype(jnp.float32), None)
    start_value = jnp.zeros((left_parts.shape[1], right_parts.shape[1]), jnp.float32)
    running, _ = lax.scan(add_group, start_value, (left_parts, right_parts))
    return running

def reference(tokens, lengths, cotangent, triple_weight, output_weight, upward_weight, downward_weight):
    row_count = tokens.shape[0]
    slates = row_count // SLATE
    model_width = tokens.shape[1]
    stream = tokens
    saved = []
    for layer_index in range(LAYERS):
        normed, scaled, rscale = normalize(stream)
        flat_triple = triple_weight[layer_index].reshape(model_width, -1)
        qkv = jnp.dot(normed, flat_triple, preferred_element_type=jnp.float32).astype(jnp.bfloat16)
        shaped = qkv.reshape(slates, SLATE, 3, HEADS, HD)
        queries = shaped[:, :, 0]
        key_rows = shaped[:, :, 1]
        values = shaped[:, :, 2]
        probs, probs_low, context = attend(queries, key_rows, values, lengths)
        context_flat = context.reshape(row_count, -1)
        attn_sum = group_total(split_groups(context_flat), split_groups(output_weight[layer_index]))
        mid_stream = (stream.astype(jnp.float32) + attn_sum).astype(jnp.bfloat16)
        normed_mid, scaled_mid, rscale_mid = normalize(mid_stream)
        preact = jnp.dot(normed_mid, upward_weight[layer_index], preferred_element_type=jnp.float32)
        activated = smooth_gate(preact).astype(jnp.bfloat16)
        ffn_sum = group_total(split_groups(activated), split_groups(downward_weight[layer_index]))
        stream = (mid_stream.astype(jnp.float32) + ffn_sum).astype(jnp.bfloat16)
        saved.append((normed, scaled, rscale, queries, key_rows, values, probs, probs_low, context_flat, scaled_mid, rscale_mid, normed_mid, preact, activated))
    final_stream = stream
    gradients = []
    upstream = cotangent
    for layer_index in reversed(range(LAYERS)):
        normed, scaled, rscale, queries, key_rows, values, probs, probs_low, context_flat, scaled_mid, rscale_mid, normed_mid, preact, activated = saved[layer_index]
        downward_grad = contract_rows(upstream, activated)
        grad_act = jnp.dot(upstream, downward_weight[layer_index], preferred_element_type=jnp.float32).astype(jnp.bfloat16)
        _, gate_back = jax.vjp(smooth_gate, preact)
        grad_preact = gate_back(grad_act.astype(jnp.float32))[0].astype(jnp.bfloat16)
        upward_grad = contract_rows(normed_mid, grad_preact)
        grad_normed = group_total(split_groups(grad_preact), split_groups(upward_weight[layer_index]))
        grad_mid = (upstream.astype(jnp.float32) + norm_backward(scaled_mid, rscale_mid, grad_normed)).astype(jnp.bfloat16)
        output_grad = contract_rows(grad_mid, context_flat)
        grad_context = jnp.dot(grad_mid, output_weight[layer_index], preferred_element_type=jnp.float32).astype(jnp.bfloat16)
        grad_query, grad_key, grad_value = attend_backward(probs, probs_low, queries, key_rows, values, grad_context.reshape(slates, SLATE, HEADS, HD))
        grad_qkv = jnp.stack([grad_query, grad_key, grad_value], axis=2).reshape(row_count, -1)
        triple_grad = contract_rows(normed, grad_qkv).reshape(model_width, 3, -1)
        gradients.insert(0, (triple_grad, output_grad, upward_grad, downward_grad))
        if layer_index > 0:
            grad_input = group_total(split_triples(grad_qkv), split_triples(triple_weight[layer_index]))
            upstream = (grad_mid.astype(jnp.float32) + norm_backward(scaled, rscale, grad_input)).astype(jnp.bfloat16)
    merged = [jnp.stack([gradients[layer_pos][slot_index] for layer_pos in range(LAYERS)]) for slot_index in range(4)]
    return (final_stream, merged[0], merged[1], merged[2], merged[3])
```

```python
import jax
import jax.numpy as jnp
from jax import lax
from jax.sharding import Mesh
from jax.sharding import PartitionSpec as P

HD = 64
SLATE = 256
LAYERS = 2
DP = ("z_lo", "y", "core")
MP = "mp"

epsilon = 1e-06
bf16 = jnp.bfloat16
f32 = jnp.float32


def share_rows(x, axis):
    n = lax.axis_size(axis)
    blocks = x.reshape(n, x.shape[0] // n, x.shape[1])
    blocks = lax.all_to_all(blocks, axis, 0, 0, tiled=True)
    return jnp.sum(blocks.astype(f32), axis=0)


def all_rows(x, axis):
    n = lax.axis_size(axis)
    copies = jnp.broadcast_to(x[None], (n, *x.shape))
    blocks = lax.all_to_all(copies, axis, 0, 0, tiled=True)
    return blocks.reshape(n * x.shape[0], x.shape[1])


def normalize(stream):
    widened = stream.astype(f32)
    rscale = lax.rsqrt(jnp.mean(widened * widened, axis=-1, keepdims=True) + epsilon)
    scaled = widened * rscale
    return (scaled.astype(bf16), scaled, rscale)


def norm_backward(scaled, rscale, upward):
    inner = jnp.mean(upward * scaled, axis=-1, keepdims=True)
    return rscale * (upward - scaled * inner)


def smooth_gate(preact):
    return jax.nn.gelu(preact, approximate=True)


def dot(left, right, dims):
    return lax.dot_general(left, right, (dims, ((), ())), preferred_element_type=f32)


def contract_rows(left, right):
    return dot(left, right, ((0,), (0,)))


def contract_cols(left, right):
    return dot(left, right, ((1,), (1,)))


def attend(queries, key_rows, values, live):
    scores = contract_cols(queries, key_rows) * HD ** (-0.5)
    weights = jnp.exp(scores) * live
    probs = weights / jnp.sum(weights, axis=-1, keepdims=True)
    context = jnp.dot(probs.astype(bf16), values, preferred_element_type=f32).astype(bf16)
    return probs, context


def attend_backward(probs, queries, key_rows, values, grad_context):
    grad_prob = contract_cols(grad_context, values)
    grad_value = contract_rows(probs.astype(bf16), grad_context).astype(bf16)
    inner = jnp.sum(grad_prob * probs, axis=-1, keepdims=True)
    grad_score = (probs * (grad_prob - inner) * HD ** (-0.5)).astype(bf16)
    grad_query = jnp.dot(grad_score, key_rows, preferred_element_type=f32).astype(bf16)
    grad_key = contract_rows(grad_score, queries).astype(bf16)
    return jnp.concatenate([grad_query, grad_key, grad_value], axis=1)


def body(tokens, lengths, cotangent, triple_weight, output_weight, upward_weight, downward_weight):
    rows, width = tokens.shape
    n = lax.axis_size(MP)
    share = rows // n
    start = lax.axis_index(MP) * share

    def part(x):
        return lax.dynamic_slice_in_dim(x, start, share, 0)

    live = (jnp.arange(SLATE)[None, :] < lengths[:, None]).astype(f32)
    triple = [triple_weight[l].reshape(width, -1) for l in range(LAYERS)]
    saved = []
    stream = tokens
    stream_part = part(tokens)
    for l in range(LAYERS):
        normed, scaled, rscale = normalize(stream)
        qkv = jnp.dot(normed, triple[l], preferred_element_type=f32).astype(bf16)
        queries, key_rows, values = (qkv[:, k * HD : (k + 1) * HD] for k in range(3))
        probs, context = attend(queries, key_rows, values, live)
        partial_att = contract_cols(context, output_weight[l]).astype(bf16)
        mid_part = (stream_part.astype(f32) + share_rows(partial_att, MP)).astype(bf16)
        mid_stream = all_rows(mid_part, MP)
        normed_mid, scaled_mid, rscale_mid = normalize(mid_stream)
        preact = jnp.dot(normed_mid, upward_weight[l], preferred_element_type=f32)
        activated = smooth_gate(preact).astype(bf16)
        partial_ffn = contract_cols(activated, downward_weight[l]).astype(bf16)
        saved.append((normed, scaled, rscale, queries, key_rows, values, probs, context,
                      scaled_mid, rscale_mid, normed_mid, preact, activated))
        if l + 1 < LAYERS:
            stream_part = (mid_part.astype(f32) + share_rows(partial_ffn, MP)).astype(bf16)
            stream = all_rows(stream_part, MP)

    reduced = [None] * LAYERS
    early = []
    upstream, upstream_part = cotangent, part(cotangent)
    for l in reversed(range(LAYERS)):
        (normed, scaled, rscale, queries, key_rows, values, probs, context,
         scaled_mid, rscale_mid, normed_mid, preact, activated) = saved[l]
        grad_act = jnp.dot(upstream, downward_weight[l], preferred_element_type=f32).astype(bf16)
        _, gate_back = jax.vjp(smooth_gate, preact)
        grad_preact = gate_back(grad_act.astype(f32))[0].astype(bf16)
        partial = contract_cols(grad_preact, upward_weight[l]).astype(bf16)
        if l + 1 == LAYERS:
            both = share_rows(jnp.concatenate([partial, partial_ffn], axis=1), MP)
            final_part = (mid_part.astype(f32) + both[:, width:]).astype(bf16)
            both = all_rows(jnp.concatenate([both[:, :width].astype(bf16), final_part], axis=1), MP)
            grad_normed, final_stream = both[:, :width].astype(f32), both[:, width:]
        else:
            grad_normed = all_rows(share_rows(partial, MP).astype(bf16), MP).astype(f32)
        downward_grad = contract_rows(upstream, activated)
        upward_grad = contract_rows(normed_mid, grad_preact)
        grad_mid = (upstream.astype(f32) + norm_backward(scaled_mid, rscale_mid, grad_normed)).astype(bf16)
        output_grad = contract_rows(grad_mid, context)
        grad_context = jnp.dot(grad_mid, output_weight[l], preferred_element_type=f32).astype(bf16)
        grad_qkv = attend_backward(probs, queries, key_rows, values, grad_context)
        triple_grad = contract_rows(normed, grad_qkv)
        early.append([upward_grad, downward_grad])
        late = [triple_grad, output_grad]
        if l > 0:
            early[-1] += late
            grad_input = all_rows(
                share_rows(contract_cols(grad_qkv, triple[l]).astype(bf16), MP).astype(bf16), MP
            ).astype(f32)
            upstream = (grad_mid.astype(f32) + norm_backward(scaled, rscale, grad_input)).astype(bf16)

    def over_slates(grads):
        joined = jnp.concatenate([g.astype(bf16) for g in grads], axis=1)
        summed = share_rows(joined, DP)
        out, at = [], 0
        for g in grads:
            out.append(summed[:, at : at + g.shape[1]])
            at += g.shape[1]
        return out

    up1, down1, triple1, out1 = over_slates(early[0])
    up0, down0 = over_slates(early[1])
    triple0, out0 = over_slates(late)
    heads = triple_weight.shape[-1]
    return (
        final_stream,
        jnp.stack([t.reshape(t.shape[0], 3, heads) for t in (triple0, triple1)]),
        jnp.stack([out0, out1]),
        jnp.stack([up0, up1]),
        jnp.stack([down0, down1]),
    )


def solution(mesh):
    torus = Mesh(mesh.devices.reshape(2, 4, 2, mesh.shape["mp"]), (*DP, MP))
    placed = (
        P(DP, None),
        P(DP),
        P(DP, None),
        P(None, None, None, MP),
        P(None, None, MP),
        P(None, None, MP),
        P(None, None, MP),
    )
    return jax.shard_map(
        body,
        mesh=torus,
        in_specs=placed,
        out_specs=(
            P(DP, None),
            P(None, DP, None, MP),
            P(None, DP, MP),
            P(None, DP, MP),
            P(None, DP, MP),
        ),
        check_vma=False,
    )
```

```python
import jax
import jax.numpy as jnp
from jax import lax
from jax.sharding import Mesh
from jax.sharding import PartitionSpec as P

HD = 64
SLATE = 256
LAYERS = 2
DP = ("z_lo", "y", "core")
MP = ("z_hi", "x")

epsilon = 1e-06
bf16 = jnp.bfloat16
f32 = jnp.float32


def share_rows(x, axis):
    n = lax.axis_size(axis)
    blocks = x.reshape(n, x.shape[0] // n, x.shape[1])
    blocks = lax.all_to_all(blocks, axis, 0, 0, tiled=True)
    return jnp.sum(blocks.astype(f32), axis=0)


def all_rows(x, axis):
    n = lax.axis_size(axis)
    copies = jnp.broadcast_to(x[None], (n, *x.shape))
    blocks = lax.all_to_all(copies, axis, 0, 0, tiled=True)
    return blocks.reshape(n * x.shape[0], x.shape[1])


def swapped(x, axis):
    return lax.ppermute(x, axis, [(0, 1), (1, 0)])


def moved(x, axis, step):
    n = lax.axis_size(axis)
    return lax.ppermute(x, axis, [(k, (k + step) % n) for k in range(n)])


def pick(x, index):
    return lax.dynamic_index_in_dim(x, index, 0, keepdims=False)


def pair_sum(x, axis):
    here = lax.axis_index(axis)
    got = swapped(pick(x, 1 - here), axis)
    return (pick(x, here).astype(f32) + got.astype(f32))


def direct_sum(x, axis):
    n = lax.axis_size(axis)
    here = lax.axis_index(axis)
    total = pick(x, here).astype(f32)
    for step in range(1, n):
        total = total + moved(pick(x, (here + step) % n), axis, step).astype(f32)
    return total


def slate_sum(grads):
    rows, cols = grads.shape
    parts = grads.reshape(2, 4, 2, rows // 16, cols)
    parts = pair_sum(jnp.moveaxis(parts, 2, 0), "core").astype(bf16)
    parts = direct_sum(jnp.moveaxis(parts, 1, 0), "y").astype(bf16)
    return pair_sum(parts, "z_lo")


def normalize(stream):
    widened = stream.astype(f32)
    rscale = lax.rsqrt(jnp.mean(widened * widened, axis=-1, keepdims=True) + epsilon)
    scaled = widened * rscale
    return (scaled.astype(bf16), scaled, rscale)


def norm_backward(scaled, rscale, upward):
    inner = jnp.mean(upward * scaled, axis=-1, keepdims=True)
    return rscale * (upward - scaled * inner)


def smooth_gate(preact):
    return jax.nn.gelu(preact, approximate=True)


def dot(left, right, dims):
    return lax.dot_general(left, right, (dims, ((), ())), preferred_element_type=f32)


def contract_rows(left, right):
    return dot(left, right, ((0,), (0,)))


def contract_cols(left, right):
    return dot(left, right, ((1,), (1,)))


def attend(queries, key_rows, values, live):
    scores = contract_cols(queries, key_rows) * HD ** (-0.5)
    weights = jnp.exp(scores) * live
    probs = weights / jnp.sum(weights, axis=-1, keepdims=True)
    context = jnp.dot(probs.astype(bf16), values, preferred_element_type=f32).astype(bf16)
    return probs, context


def attend_backward(probs, queries, key_rows, values, grad_context):
    grad_prob = contract_cols(grad_context, values)
    grad_value = contract_rows(probs.astype(bf16), grad_context).astype(bf16)
    inner = jnp.sum(grad_prob * probs, axis=-1, keepdims=True)
    grad_score = (probs * (grad_prob - inner) * HD ** (-0.5)).astype(bf16)
    grad_query = jnp.dot(grad_score, key_rows, preferred_element_type=f32).astype(bf16)
    grad_key = contract_rows(grad_score, queries).astype(bf16)
    return jnp.concatenate([grad_query, grad_key, grad_value], axis=1)


def body(tokens, lengths, cotangent, triple_weight, output_weight, upward_weight, downward_weight):
    rows, width = tokens.shape
    n = lax.axis_size(MP)
    share = rows // n
    start = lax.axis_index(MP) * share

    def part(x):
        return lax.dynamic_slice_in_dim(x, start, share, 0)

    live = (jnp.arange(SLATE)[None, :] < lengths[:, None]).astype(f32)
    triple = [triple_weight[l].reshape(width, -1) for l in range(LAYERS)]
    saved = []
    stream = tokens
    stream_part = part(tokens)
    for l in range(LAYERS):
        normed, scaled, rscale = normalize(stream)
        qkv = jnp.dot(normed, triple[l], preferred_element_type=f32).astype(bf16)
        queries, key_rows, values = (qkv[:, k * HD : (k + 1) * HD] for k in range(3))
        probs, context = attend(queries, key_rows, values, live)
        partial_att = contract_cols(context, output_weight[l]).astype(bf16)
        mid_part = (stream_part.astype(f32) + share_rows(partial_att, MP)).astype(bf16)
        mid_stream = all_rows(mid_part, MP)
        normed_mid, scaled_mid, rscale_mid = normalize(mid_stream)
        preact = jnp.dot(normed_mid, upward_weight[l], preferred_element_type=f32)
        activated = smooth_gate(preact).astype(bf16)
        partial_ffn = contract_cols(activated, downward_weight[l]).astype(bf16)
        saved.append((normed, scaled, rscale, queries, key_rows, values, probs, context,
                      scaled_mid, rscale_mid, normed_mid, preact, activated))
        if l + 1 < LAYERS:
            stream_part = (mid_part.astype(f32) + share_rows(partial_ffn, MP)).astype(bf16)
            stream = all_rows(stream_part, MP)

    early = []
    upstream = cotangent
    for l in reversed(range(LAYERS)):
        (normed, scaled, rscale, queries, key_rows, values, probs, context,
         scaled_mid, rscale_mid, normed_mid, preact, activated) = saved[l]
        grad_act = jnp.dot(upstream, downward_weight[l], preferred_element_type=f32).astype(bf16)
        _, gate_back = jax.vjp(smooth_gate, preact)
        grad_preact = gate_back(grad_act.astype(f32))[0].astype(bf16)
        partial = contract_cols(grad_preact, upward_weight[l]).astype(bf16)
        if l + 1 == LAYERS:
            quarter = width // lax.axis_size("x")
            shares = jnp.stack([partial_ffn[:, k * quarter : (k + 1) * quarter] for k in range(4)])
            shares = direct_sum(shares, "x").astype(bf16).reshape(n, share, quarter)
            own = share_rows(partial, MP).astype(bf16)
            sent = jnp.concatenate([jnp.broadcast_to(own[None], (n, share, width)), shares], axis=2)
            came = lax.all_to_all(sent, MP, 0, 0, tiled=True)
            grad_normed = came[:, :, :width].reshape(rows, width).astype(f32)
            ffn_part = jnp.sum(came[:, :, width:].reshape(4, 4, share, quarter).astype(f32), axis=0)
            ffn_part = jnp.concatenate([ffn_part[k] for k in range(4)], axis=1)
            final_part = (mid_part.astype(f32) + ffn_part).astype(bf16)
        else:
            grad_normed = all_rows(share_rows(partial, MP).astype(bf16), MP).astype(f32)
        downward_grad = contract_rows(upstream, activated)
        upward_grad = contract_rows(normed_mid, grad_preact)
        grad_mid = (upstream.astype(f32) + norm_backward(scaled_mid, rscale_mid, grad_normed)).astype(bf16)
        output_grad = contract_rows(grad_mid, context)
        grad_context = jnp.dot(grad_mid, output_weight[l], preferred_element_type=f32).astype(bf16)
        grad_qkv = attend_backward(probs, queries, key_rows, values, grad_context)
        triple_grad = contract_rows(normed, grad_qkv)
        early.append([upward_grad, downward_grad])
        late = [triple_grad, output_grad]
        if l > 0:
            early[-1] += late
            partial = contract_cols(grad_qkv, triple[l]).astype(bf16).reshape(n, share, width)
            quarters = jnp.stack([final_part[:, k * quarter : (k + 1) * quarter] for k in range(4)])
            sent = jnp.concatenate([partial, jnp.tile(quarters, (4, 1, 1))], axis=2)
            came = lax.all_to_all(sent, MP, 0, 0, tiled=True)
            own = jnp.sum(came[:, :, :width].astype(f32), axis=0).astype(bf16)
            column = came[:, :, width:].reshape(rows, quarter)
            here = lax.axis_index("x")
            columns = [column] + [moved(column, "x", step) for step in range(1, 4)]
            final_stream = jnp.concatenate(
                [
                    lax.select_n((here - k) % 4, *columns)
                    for k in range(4)
                ],
                axis=1,
            )
            grad_input = all_rows(own, MP).astype(f32)
            upstream = (grad_mid.astype(f32) + norm_backward(scaled, rscale, grad_input)).astype(bf16)

    def over_slates(grads, total):
        joined = jnp.concatenate([g.astype(bf16) for g in grads], axis=1)
        summed = total(joined)
        out, at = [], 0
        for g in grads:
            out.append(summed[:, at : at + g.shape[1]])
            at += g.shape[1]
        return out

    up1, down1, triple1, out1 = over_slates(early[0], slate_sum)
    up0, down0 = over_slates(early[1], slate_sum)
    triple0, out0 = over_slates(late, lambda g: share_rows(g, DP))
    heads = triple_weight.shape[-1]
    return (
        final_stream,
        jnp.stack([t.reshape(t.shape[0], 3, heads) for t in (triple0, triple1)]),
        jnp.stack([out0, out1]),
        jnp.stack([up0, up1]),
        jnp.stack([down0, down1]),
    )


def solution(mesh):
    torus = Mesh(mesh.devices.reshape(2, 4, 2, 4, 4), (*DP, *MP))
    placed = (
        P(DP, None),
        P(DP),
        P(DP, None),
        P(None, None, None, MP),
        P(None, None, MP),
        P(None, None, MP),
        P(None, None, MP),
    )
    return jax.shard_map(
        body,
        mesh=torus,
        in_specs=placed,
        out_specs=(
            P(DP, None),
            P(None, DP, None, MP),
            P(None, DP, MP),
            P(None, DP, MP),
            P(None, DP, MP),
        ),
        check_vma=False,
    )
```

```python
import jax
import jax.numpy as jnp
from jax import lax
from jax.sharding import Mesh
from jax.sharding import PartitionSpec as P


HD = 64
SLATE = 256
LAYERS = 2
DP = ("z_lo", "y", "core")
MP = ("z_hi", "x")

epsilon = 1e-06
bf16 = jnp.bfloat16
f32 = jnp.float32


def share_rows(x, axis):
    n = lax.axis_size(axis)
    blocks = x.reshape(n, x.shape[0] // n, x.shape[1])
    blocks = lax.all_to_all(blocks, axis, 0, 0, tiled=True)
    return jnp.sum(blocks.astype(f32), axis=0)


def all_rows(x, axis):
    n = lax.axis_size(axis)
    copies = jnp.broadcast_to(x[None], (n, *x.shape))
    blocks = lax.all_to_all(copies, axis, 0, 0, tiled=True)
    return blocks.reshape(n * x.shape[0], x.shape[1])


def after(x, *others):
    return lax.optimization_barrier((x, *others))[0]


def swapped(x, axis):
    return lax.ppermute(x, axis, [(0, 1), (1, 0)])


def moved(x, axis, step):
    n = lax.axis_size(axis)
    return lax.ppermute(x, axis, [(k, (k + step) % n) for k in range(n)])


def pick(x, index):
    return lax.dynamic_index_in_dim(x, index, 0, keepdims=False)


def core_stage(grads):
    rows, _ = grads[0].shape
    joined = jnp.concatenate([g.astype(bf16) for g in grads], axis=1)
    parts = joined.reshape(8, 2, rows // 16, cols_of(grads))
    return pair_parts(jnp.moveaxis(parts, 1, 0), "core")


def cols_of(arrays):
    return sum(a.shape[1] for a in arrays)


def pair_parts(x, axis):
    here = lax.axis_index(axis)
    return pick(x, here), swapped(pick(x, 1 - here), axis)


def total(parts):
    return sum(p.astype(f32) for p in parts)


def y_stage(parts):
    parts = jnp.moveaxis(parts.reshape(2, 4, *parts.shape[1:]), 1, 0)
    here = lax.axis_index("y")
    return [pick(parts, here)] + [moved(pick(parts, (here + k) % 4), "y", k) for k in range(1, 4)]


def normalize(stream):
    widened = stream.astype(f32)
    rscale = lax.rsqrt(jnp.mean(widened * widened, axis=-1, keepdims=True) + epsilon)
    scaled = widened * rscale
    return (scaled.astype(bf16), scaled, rscale)


def norm_backward(scaled, rscale, upward):
    inner = jnp.mean(upward * scaled, axis=-1, keepdims=True)
    return rscale * (upward - scaled * inner)


def smooth_gate(preact):
    return jax.nn.gelu(preact, approximate=True)


def dot(left, right, dims):
    return lax.dot_general(left, right, (dims, ((), ())), preferred_element_type=f32)


def contract_rows(left, right):
    return dot(left, right, ((0,), (0,)))


def contract_cols(left, right):
    return dot(left, right, ((1,), (1,)))


def attend(queries, key_rows, values, live):
    scores = contract_cols(queries, key_rows) * HD ** (-0.5)
    weights = jnp.exp(scores) * live
    probs = weights / jnp.sum(weights, axis=-1, keepdims=True)
    context = jnp.dot(probs.astype(bf16), values, preferred_element_type=f32).astype(bf16)
    return probs, context


def attend_backward(probs, queries, key_rows, values, grad_context):
    grad_prob = contract_cols(grad_context, values)
    grad_value = contract_rows(probs.astype(bf16), grad_context).astype(bf16)
    inner = jnp.sum(grad_prob * probs, axis=-1, keepdims=True)
    grad_score = (probs * (grad_prob - inner) * HD ** (-0.5)).astype(bf16)
    grad_query = jnp.dot(grad_score, key_rows, preferred_element_type=f32).astype(bf16)
    grad_key = contract_rows(grad_score, queries).astype(bf16)
    return jnp.concatenate([grad_query, grad_key, grad_value], axis=1)


def step(tokens, lengths, cotangent, triple_weight, output_weight, upward_weight, downward_weight):
    rows, width = tokens.shape
    n = lax.axis_size(MP)
    share = rows // n
    start = lax.axis_index(MP) * share

    def part(x):
        return lax.dynamic_slice_in_dim(x, start, share, 0)

    live = (jnp.arange(SLATE)[None, :] < lengths[:, None]).astype(f32)
    triple = [triple_weight[l].reshape(width, -1) for l in range(LAYERS)]
    saved = []
    stream = tokens
    stream_part = part(tokens)
    for l in range(LAYERS):
        normed, scaled, rscale = normalize(stream)
        qkv = jnp.dot(normed, triple[l], preferred_element_type=f32).astype(bf16)
        queries, key_rows, values = (qkv[:, k * HD : (k + 1) * HD] for k in range(3))
        probs, context = attend(queries, key_rows, values, live)
        partial_att = contract_cols(context, output_weight[l]).astype(bf16)
        mid_part = (stream_part.astype(f32) + share_rows(partial_att, MP)).astype(bf16)
        mid_stream = all_rows(mid_part, MP)
        normed_mid, scaled_mid, rscale_mid = normalize(mid_stream)
        preact = jnp.dot(normed_mid, upward_weight[l], preferred_element_type=f32)
        activated = smooth_gate(preact).astype(bf16)
        partial_ffn = contract_cols(activated, downward_weight[l]).astype(bf16)
        saved.append((normed, scaled, rscale, queries, key_rows, values, probs, context,
                      scaled_mid, rscale_mid, normed_mid, preact, activated))
        if l + 1 < LAYERS:
            stream_part = (mid_part.astype(f32) + share_rows(partial_ffn, MP)).astype(bf16)
            stream = all_rows(stream_part, MP)

    top = LAYERS - 1
    quarter = width // 4
    heads = triple_weight.shape[-1]
    x_here = lax.axis_index("x")

    (normed, scaled, rscale, queries, key_rows, values, probs, context,
     scaled_mid, rscale_mid, normed_mid, preact, activated) = saved[top]
    upstream = cotangent
    grad_act = jnp.dot(upstream, downward_weight[top], preferred_element_type=f32).astype(bf16)
    _, gate_back = jax.vjp(smooth_gate, preact)
    grad_preact = gate_back(grad_act.astype(f32))[0].astype(bf16)
    partial = contract_cols(grad_preact, upward_weight[top]).astype(bf16)
    shares = jnp.stack([partial_ffn[:, k * quarter : (k + 1) * quarter] for k in range(4)])
    shares = [pick(shares, x_here)] + [
        moved(pick(shares, (x_here + k) % 4), "x", k) for k in range(1, 4)
    ]
    own = share_rows(partial, MP).astype(bf16)
    shares = total(shares).astype(bf16).reshape(n, share, quarter)
    sent = jnp.concatenate([jnp.broadcast_to(own[None], (n, share, width)), shares], axis=2)
    came = lax.all_to_all(after(sent, rscale_mid), MP, 0, 0, tiled=True)
    grad_normed = came[:, :, :width].reshape(rows, width).astype(f32)
    ffn_part = jnp.sum(came[:, :, width:].reshape(4, 4, share, quarter).astype(f32), axis=0)
    ffn_part = jnp.concatenate([ffn_part[k] for k in range(4)], axis=1)
    final_part = (mid_part.astype(f32) + ffn_part).astype(bf16)
    grad_mid = (upstream.astype(f32) + norm_backward(scaled_mid, rscale_mid, grad_normed)).astype(bf16)
    grad_context = jnp.dot(grad_mid, output_weight[top], preferred_element_type=f32).astype(bf16)
    grad_qkv = attend_backward(probs, queries, key_rows, values, grad_context)
    partial = contract_cols(grad_qkv, triple[top]).astype(bf16).reshape(n, share, width)
    quarters = jnp.stack([final_part[:, k * quarter : (k + 1) * quarter] for k in range(4)])
    sent = jnp.concatenate([partial, jnp.tile(quarters, (4, 1, 1))], axis=2)
    came = lax.all_to_all(sent, MP, 0, 0, tiled=True)
    own = jnp.sum(came[:, :, :width].astype(f32), axis=0).astype(bf16)
    column = came[:, :, width:].reshape(rows, quarter)
    wide1 = [
        contract_rows(normed_mid, grad_preact),
        contract_rows(upstream, activated),
        contract_rows(normed, grad_qkv),
        contract_rows(grad_mid, context),
    ]
    sums1 = core_stage(wide1)
    grad_input = all_rows(after(own, rscale, sums1[0]), MP).astype(f32)
    sums1 = y_stage(total(sums1).astype(bf16))
    grad_input = after(grad_input, sums1[0])
    upstream = (grad_mid.astype(f32) + norm_backward(scaled, rscale, grad_input)).astype(bf16)
    (normed, scaled, rscale, queries, key_rows, values, probs, context,
     scaled_mid, rscale_mid, normed_mid, preact, activated) = saved[0]
    grad_act = jnp.dot(upstream, downward_weight[0], preferred_element_type=f32).astype(bf16)
    _, gate_back = jax.vjp(smooth_gate, preact)
    grad_preact = gate_back(grad_act.astype(f32))[0].astype(bf16)
    partial = contract_cols(grad_preact, upward_weight[0]).astype(bf16)
    own = share_rows(partial, MP).astype(bf16)
    wide0 = [contract_rows(normed_mid, grad_preact), contract_rows(upstream, activated)]
    sums0 = core_stage(wide0)
    sums1 = pair_parts(total(sums1).astype(bf16), "z_lo")
    grad_normed = all_rows(after(own, rscale_mid, sums0[0], sums1[0]), MP).astype(f32)
    sums0 = y_stage(total(sums0).astype(bf16))
    grad_normed = after(grad_normed, sums0[0])
    grad_mid = (upstream.astype(f32) + norm_backward(scaled_mid, rscale_mid, grad_normed)).astype(bf16)
    grad_context = jnp.dot(grad_mid, output_weight[0], preferred_element_type=f32).astype(bf16)
    grad_qkv = attend_backward(probs, queries, key_rows, values, grad_context)
    late = [contract_rows(normed, grad_qkv), contract_rows(grad_mid, context)]
    late = jnp.concatenate([g.astype(bf16) for g in late], axis=1)
    column = after(column, late)
    columns = [column] + [moved(column, "x", step) for step in range(1, 4)]
    late = share_rows(late, DP)
    sums0 = pair_parts(total(sums0).astype(bf16), "z_lo")
    final_stream = jnp.concatenate(
        [lax.select_n((x_here - k) % 4, *columns) for k in range(4)], axis=1
    )
    sums1, sums0 = total(sums1), total(sums0)

    def cut(x, first, size):
        return x[:, first : first + size]

    ff = upward_weight.shape[-1]
    return (
        final_stream,
        jnp.stack([
            cut(late, 0, 3 * heads).reshape(-1, 3, heads),
            cut(sums1, 2 * ff, 3 * heads).reshape(-1, 3, heads),
        ]),
        jnp.stack([cut(late, 3 * heads, heads), cut(sums1, 2 * ff + 3 * heads, heads)]),
        jnp.stack([cut(sums0, 0, ff), cut(sums1, 0, ff)]),
        jnp.stack([cut(sums0, ff, ff), cut(sums1, ff, ff)]),
    )


def solution(mesh):
    torus = Mesh(mesh.devices.reshape(2, 4, 2, 4, 4), (*DP, *MP))
    placed = (
        P(DP, None),
        P(DP),
        P(DP, None),
        P(None, None, None, MP),
        P(None, None, MP),
        P(None, None, MP),
        P(None, None, MP),
    )
    return jax.shard_map(
        step,
        mesh=torus,
        in_specs=placed,
        out_specs=(
            P(DP, None),
            P(None, DP, None, MP),
            P(None, DP, MP),
            P(None, DP, MP),
            P(None, DP, MP),
        ),
        check_vma=False,
    )
```

```python
import jax
import jax.numpy as jnp
from jax import lax
from jax.sharding import Mesh
from jax.sharding import PartitionSpec as P


HD = 64
SLATE = 256
LAYERS = 2
DP = ("z_lo", "y", "core")
MP = ("z_hi", "x")


epsilon = 1e-06
bf16 = jnp.bfloat16
f32 = jnp.float32


def share_rows(x, axis):
    n = lax.axis_size(axis)
    blocks = x.reshape(n, x.shape[0] // n, x.shape[1])
    blocks = lax.all_to_all(blocks, axis, 0, 0, tiled=True)
    return jnp.sum(blocks.astype(f32), axis=0)


def all_rows(x, axis):
    n = lax.axis_size(axis)
    copies = jnp.broadcast_to(x[None], (n, *x.shape))
    blocks = lax.all_to_all(copies, axis, 0, 0, tiled=True)
    return blocks.reshape(n * x.shape[0], x.shape[1])


def after(x, *others):
    return lax.optimization_barrier((x, *others))[0]


def moved(x, axis, step):
    n = lax.axis_size(axis)
    return lax.ppermute(x, axis, [(k, (k + step) % n) for k in range(n)])


def pick(x, index):
    return lax.dynamic_index_in_dim(x, index, 0, keepdims=False)


def total(parts):
    return sum(p.astype(f32) for p in parts)


def y_stage(grads):
    joined = jnp.concatenate([g.astype(bf16) for g in grads], axis=1)
    rows, cols = joined.shape
    parts = jnp.moveaxis(joined.reshape(2, 4, 2, rows // 16, cols), 1, 0)
    here = lax.axis_index("y")
    sent = [pick(parts, (here + k) % 4) for k in range(1, 4)]
    return [pick(parts, here)] + [moved(s, "y", k) for k, s in enumerate(sent, 1)], sent


def quad_stage(parts):
    axes = ("z_lo", "core")
    here = lax.axis_index(axes)
    return [pick(parts, here)] + [
        lax.ppermute(pick(parts, here ^ k), axes, [(i, i ^ k) for i in range(4)]) for k in range(1, 4)
    ]


def normalize(stream):
    widened = stream.astype(f32)
    rscale = lax.rsqrt(jnp.mean(widened * widened, axis=-1, keepdims=True) + epsilon)
    scaled = widened * rscale
    return (scaled.astype(bf16), scaled, rscale)


def norm_backward(scaled, rscale, upward):
    inner = jnp.mean(upward * scaled, axis=-1, keepdims=True)
    return rscale * (upward - scaled * inner)


def norm_added(upstream, stream, grad):
    _, scaled, rscale = normalize(stream)
    return (upstream.astype(f32) + norm_backward(scaled, rscale, grad)).astype(bf16)


def smooth_gate(preact):
    return jax.nn.gelu(preact, approximate=True)


def dot(left, right, dims):
    return lax.dot_general(left, right, (dims, ((), ())), preferred_element_type=f32)


def contract_rows(left, right):
    return dot(left, right, ((0,), (0,)))


def contract_cols(left, right):
    return dot(left, right, ((1,), (1,)))


def attend(queries, key_rows, values, live):
    scores = contract_cols(queries, key_rows) * HD ** (-0.5)
    weights = jnp.exp(scores) * live
    probs = weights / jnp.sum(weights, axis=-1, keepdims=True)
    context = jnp.dot(probs.astype(bf16), values, preferred_element_type=f32).astype(bf16)
    return probs, context


def attend_backward(probs, queries, key_rows, values, grad_context):
    grad_prob = contract_cols(grad_context, values)
    grad_value = contract_rows(probs.astype(bf16), grad_context).astype(bf16)
    inner = jnp.sum(grad_prob * probs, axis=-1, keepdims=True)
    grad_score = (probs * (grad_prob - inner) * HD ** (-0.5)).astype(bf16)
    grad_query = jnp.dot(grad_score, key_rows, preferred_element_type=f32).astype(bf16)
    grad_key = contract_rows(grad_score, queries).astype(bf16)
    return jnp.concatenate([grad_query, grad_key, grad_value], axis=1)


def step(tokens, lengths, cotangent, triple_weight, output_weight, upward_weight, downward_weight):
    rows, width = tokens.shape
    n = lax.axis_size(MP)
    share = rows // n
    start = lax.axis_index(MP) * share

    def part(x):
        return lax.dynamic_slice_in_dim(x, start, share, 0)

    live = (jnp.arange(SLATE)[None, :] < lengths[:, None]).astype(f32)
    triple = [triple_weight[l].reshape(width, -1) for l in range(LAYERS)]
    saved, owned = [], []
    stream = tokens
    stream_part = part(tokens)
    for l in range(LAYERS):
        normed = normalize(stream)[0]
        qkv = jnp.dot(normed, triple[l], preferred_element_type=f32).astype(bf16)
        queries, key_rows, values = (qkv[:, k * HD : (k + 1) * HD] for k in range(3))
        probs, context = attend(queries, key_rows, values, live)
        partial_att = contract_cols(context, output_weight[l]).astype(bf16)
        mid_part = (stream_part.astype(f32) + share_rows(partial_att, MP)).astype(bf16)
        mid_stream = all_rows(mid_part, MP)
        normed_mid = normalize(mid_stream)[0]
        preact = jnp.dot(normed_mid, upward_weight[l], preferred_element_type=f32)
        activated = smooth_gate(preact).astype(bf16)
        partial_ffn = contract_cols(activated, downward_weight[l]).astype(bf16)
        saved.append((normed, queries, key_rows, values, probs, context, normed_mid, preact, activated))
        owned.append((stream_part, mid_part))
        if l + 1 < LAYERS:
            stream_part = (mid_part.astype(f32) + share_rows(partial_ffn, MP)).astype(bf16)
            stream = all_rows(stream_part, MP)

    top = LAYERS - 1
    quarter = width // 4
    heads = triple_weight.shape[-1]
    x_here = lax.axis_index("x")

    normed, queries, key_rows, values, probs, context, normed_mid, preact, activated = saved[top]
    stream_part, mid_part = owned[top]
    upstream, upstream_part = cotangent, part(cotangent)
    grad_act = jnp.dot(upstream, downward_weight[top], preferred_element_type=f32).astype(bf16)
    _, gate_back = jax.vjp(smooth_gate, preact)
    grad_preact = gate_back(grad_act.astype(f32))[0].astype(bf16)
    partial = contract_cols(grad_preact, upward_weight[top]).astype(bf16)
    shares = jnp.stack([partial_ffn[:, k * quarter : (k + 1) * quarter] for k in range(4)])
    shares = [pick(shares, x_here)] + [
        moved(pick(shares, (x_here + k) % 4), "x", k) for k in range(1, 4)
    ]
    grad_normed = share_rows(partial, MP)
    own = upstream_part = norm_added(upstream_part, mid_part, grad_normed)
    shares = total(shares).astype(bf16).reshape(n, share, quarter)
    sent = jnp.concatenate([jnp.broadcast_to(own[None], (n, share, width)), shares], axis=2)
    came = lax.all_to_all(sent, MP, 0, 0, tiled=True)
    grad_mid = came[:, :, :width].reshape(rows, width)
    ffn_part = jnp.sum(came[:, :, width:].reshape(4, 4, share, quarter).astype(f32), axis=0)
    ffn_part = jnp.concatenate([ffn_part[k] for k in range(4)], axis=1)
    final_part = (mid_part.astype(f32) + ffn_part).astype(bf16)
    grad_context = jnp.dot(grad_mid, output_weight[top], preferred_element_type=f32).astype(bf16)
    grad_qkv = attend_backward(probs, queries, key_rows, values, grad_context)
    partial = contract_cols(grad_qkv, triple[top]).astype(bf16).reshape(n, share, width)
    quarters = jnp.stack([final_part[:, k * quarter : (k + 1) * quarter] for k in range(4)])
    sent = jnp.concatenate([partial, jnp.tile(quarters, (4, 1, 1))], axis=2)
    came = lax.all_to_all(sent, MP, 0, 0, tiled=True)
    grad_input = jnp.sum(came[:, :, :width].astype(f32), axis=0)
    own = upstream_part = norm_added(upstream_part, stream_part, grad_input)
    column = came[:, :, width:].reshape(rows, quarter)
    wide1 = [
        contract_rows(normed_mid, grad_preact),
        contract_rows(upstream, activated),
        contract_rows(normed, grad_qkv),
        contract_rows(grad_mid, context),
    ]
    sums1, sent1 = y_stage(wide1)
    upstream = all_rows(after(own, *sent1), MP)
    normed, queries, key_rows, values, probs, context, normed_mid, preact, activated = saved[0]
    mid_part = owned[0][1]
    grad_act = jnp.dot(upstream, downward_weight[0], preferred_element_type=f32).astype(bf16)
    _, gate_back = jax.vjp(smooth_gate, preact)
    grad_preact = gate_back(grad_act.astype(f32))[0].astype(bf16)
    partial = contract_cols(grad_preact, upward_weight[0]).astype(bf16)
    grad_normed = share_rows(partial, MP)
    own = norm_added(upstream_part, mid_part, grad_normed)
    wide0 = [contract_rows(normed_mid, grad_preact), contract_rows(upstream, activated)]
    sums0, sent0 = y_stage(wide0)
    grad_mid = all_rows(after(own, *sent0), MP)
    grad_context = jnp.dot(grad_mid, output_weight[0], preferred_element_type=f32).astype(bf16)
    grad_qkv = attend_backward(probs, queries, key_rows, values, grad_context)
    late = [contract_rows(normed, grad_qkv), contract_rows(grad_mid, context)]
    late = jnp.concatenate([g.astype(bf16) for g in late], axis=1)
    column = after(column, late)
    columns = [column] + [moved(column, "x", step) for step in range(1, 4)]
    sums1 = total(sums1).astype(bf16)
    sums0 = total(sums0).astype(bf16)
    sums = jnp.concatenate([sums1, sums0], axis=3)
    sums = quad_stage(sums.reshape(4, *sums.shape[2:]))
    late = share_rows(late, DP)
    final_stream = jnp.concatenate(
        [lax.select_n((x_here - k) % 4, *columns) for k in range(4)], axis=1
    )
    sums = total(sums)

    def cut(x, first, size):
        return x[:, first : first + size]

    ff = upward_weight.shape[-1]
    first0 = 2 * ff + 4 * heads
    return (
        final_stream,
        jnp.stack([
            cut(late, 0, 3 * heads).reshape(-1, 3, heads),
            cut(sums, 2 * ff, 3 * heads).reshape(-1, 3, heads),
        ]),
        jnp.stack([cut(late, 3 * heads, heads), cut(sums, 2 * ff + 3 * heads, heads)]),
        jnp.stack([cut(sums, first0, ff), cut(sums, 0, ff)]),
        jnp.stack([cut(sums, first0 + ff, ff), cut(sums, ff, ff)]),
    )


def solution(mesh):
    torus = Mesh(mesh.devices.reshape(2, 4, 2, 4, 4), (*DP, *MP))
    placed = (
        P(DP, None),
        P(DP),
        P(DP, None),
        P(None, None, None, MP),
        P(None, None, MP),
        P(None, None, MP),
        P(None, None, MP),
    )
    return jax.shard_map(
        step,
        mesh=torus,
        in_specs=placed,
        out_specs=(
            P(DP, None),
            P(None, DP, None, MP),
            P(None, DP, MP),
            P(None, DP, MP),
            P(None, DP, MP),
        ),
        check_vma=False,
    )
```

```python
import jax
import jax.numpy as jnp
from jax import lax
from jax.sharding import Mesh
from jax.sharding import PartitionSpec as P


HD = 64
SLATE = 256
LAYERS = 2
DP = ("z_lo", "y", "core")
MP = ("z_hi", "x")
QUAD = ("z_lo", "core")


epsilon = 1e-06
bf16 = jnp.bfloat16
f32 = jnp.float32


def share_rows(x, axis):
    n = lax.axis_size(axis)
    blocks = x.reshape(n, x.shape[0] // n, x.shape[1])
    blocks = lax.all_to_all(blocks, axis, 0, 0, tiled=True)
    return jnp.sum(blocks.astype(f32), axis=0)


def all_rows(x, axis):
    n = lax.axis_size(axis)
    copies = jnp.broadcast_to(x[None], (n, *x.shape))
    blocks = lax.all_to_all(copies, axis, 0, 0, tiled=True)
    return blocks.reshape(n * x.shape[0], x.shape[1])


def after(x, *others):
    return lax.optimization_barrier((x, *others))[0]


def moved(x, axis, step):
    n = lax.axis_size(axis)
    return lax.ppermute(x, axis, [(k, (k + step) % n) for k in range(n)])


def unsigned(index):
    return index.astype(jnp.uint32)


def pick(x, index):
    return lax.dynamic_slice_in_dim(x, index, 1, 0)[0]


def total(parts):
    return sum(p.astype(f32) for p in parts)


def y_stage(grads, turns):
    joined = jnp.concatenate([g.astype(bf16) for g in grads], axis=1)
    rows, cols = joined.shape
    parts = jnp.moveaxis(joined.reshape(2, 4, 2, rows // 16, cols), 1, 0)
    sent = [pick(parts, turns[k]) for k in range(1, 4)]
    return [pick(parts, turns[0])] + [moved(s, "y", k) for k, s in enumerate(sent, 1)], sent


def quad_stage(parts, turns):
    return [pick(parts, turns[0])] + [
        lax.ppermute(pick(parts, turns[k]), QUAD, [(i, i ^ k) for i in range(4)]) for k in range(1, 4)
    ]


def normalize(stream):
    widened = stream.astype(f32)
    rscale = lax.rsqrt(jnp.mean(widened * widened, axis=-1, keepdims=True) + epsilon)
    return lax.optimization_barrier((widened * rscale).astype(bf16))


def norm_backward(stream, upward):
    widened = after(stream, upward).astype(f32)
    upward = upward.astype(f32)
    rscale = lax.rsqrt(jnp.mean(widened * widened, axis=-1, keepdims=True) + epsilon)
    inner = rscale * jnp.mean(upward * widened, axis=-1, keepdims=True)
    return rscale * (upward - widened * rscale * inner)


def smooth_gate(preact):
    return jax.nn.gelu(preact, approximate=True)


def dot(left, right, dims):
    return lax.dot_general(left, right, (dims, ((), ())), preferred_element_type=f32)


def contract_rows(left, right):
    return dot(left, right, ((0,), (0,)))


def contract_cols(left, right):
    return dot(left, right, ((1,), (1,)))


def attend(queries, key_rows, values, live):
    scores = contract_cols(queries, key_rows) * HD ** (-0.5)
    weights = jnp.exp(scores) * live
    probs = weights / jnp.sum(weights, axis=-1, keepdims=True)
    context = jnp.dot(probs.astype(bf16), values, preferred_element_type=f32).astype(bf16)
    return probs, context


def attend_backward(probs, queries, key_rows, values, grad_context):
    grad_prob = contract_cols(grad_context, values)
    grad_value = contract_rows(probs.astype(bf16), grad_context).astype(bf16)
    inner = jnp.sum(grad_prob * probs, axis=-1, keepdims=True)
    grad_score = (probs * (grad_prob - inner) * HD ** (-0.5)).astype(bf16)
    grad_query = jnp.dot(grad_score, key_rows, preferred_element_type=f32).astype(bf16)
    grad_key = contract_rows(grad_score, queries).astype(bf16)
    return jnp.concatenate([grad_query, grad_key, grad_value], axis=1)


def step(tokens, lengths, cotangent, triple_weight, output_weight, upward_weight, downward_weight):
    rows, width = tokens.shape
    n = lax.axis_size(MP)
    share = rows // n
    x_here, y_here, quad_here = (unsigned(lax.axis_index(a)) for a in ("x", "y", QUAD))
    start, *places = lax.optimization_barrier((
        unsigned(lax.axis_index(MP) * share),
        *((x_here + k) & 3 for k in range(4)),
        *((x_here - k) & 3 for k in range(4)),
        *((y_here + k) & 3 for k in range(4)),
        *(quad_here ^ k for k in range(4)),
    ))
    x_turns, x_slots, y_turns, quad_turns = (places[k : k + 4] for k in range(0, 16, 4))

    def part(x):
        return lax.dynamic_slice_in_dim(x, start, share, 0)

    live = (jnp.arange(SLATE)[None, :] < lengths[:, None]).astype(f32)
    triple = [triple_weight[l].reshape(width, -1) for l in range(LAYERS)]
    saved = []
    stream = tokens
    stream_part = part(tokens)
    for l in range(LAYERS):
        normed = normalize(stream)
        qkv = jnp.dot(normed, triple[l], preferred_element_type=f32).astype(bf16)
        queries, key_rows, values = (qkv[:, k * HD : (k + 1) * HD] for k in range(3))
        probs, context = attend(queries, key_rows, values, live)
        partial_att = contract_cols(context, output_weight[l]).astype(bf16)
        if l == 0:
            partial_att = after(partial_att, *places)
        mid_part = (stream_part.astype(f32) + share_rows(partial_att, MP)).astype(bf16)
        mid_stream = all_rows(mid_part, MP)
        normed_mid = normalize(mid_stream)
        preact = jnp.dot(normed_mid, upward_weight[l], preferred_element_type=f32)
        activated = smooth_gate(preact).astype(bf16)
        partial_ffn = contract_cols(activated, downward_weight[l]).astype(bf16)
        saved.append((normed, stream, queries, key_rows, values, probs, context,
                      mid_stream, normed_mid, preact, activated))
        if l + 1 < LAYERS:
            stream_part = (mid_part.astype(f32) + share_rows(partial_ffn, MP)).astype(bf16)
            stream = all_rows(stream_part, MP)

    top = LAYERS - 1
    quarter = width // 4
    heads = triple_weight.shape[-1]

    (normed, stream, queries, key_rows, values, probs, context,
     mid_stream, normed_mid, preact, activated) = saved[top]
    upstream = cotangent
    grad_act = jnp.dot(upstream, downward_weight[top], preferred_element_type=f32).astype(bf16)
    _, gate_back = jax.vjp(smooth_gate, preact)
    grad_preact = gate_back(grad_act.astype(f32))[0].astype(bf16)
    partial = contract_cols(grad_preact, upward_weight[top]).astype(bf16)
    shares = jnp.stack([partial_ffn[:, k * quarter : (k + 1) * quarter] for k in range(4)])
    shares = [pick(shares, x_turns[0])] + [
        moved(pick(shares, x_turns[k]), "x", k) for k in range(1, 4)
    ]
    own = share_rows(partial, MP).astype(bf16)
    shares = total(shares).astype(bf16).reshape(n, share, quarter)
    sent = jnp.concatenate([jnp.broadcast_to(own[None], (n, share, width)), shares], axis=2)
    came = lax.all_to_all(sent, MP, 0, 0, tiled=True)
    grad_normed = came[:, :, :width].reshape(rows, width)
    ffn_part = jnp.sum(came[:, :, width:].reshape(4, 4, share, quarter).astype(f32), axis=0)
    ffn_part = jnp.concatenate([ffn_part[k] for k in range(4)], axis=1)
    final_part = (mid_part.astype(f32) + ffn_part).astype(bf16)
    grad_mid = (upstream.astype(f32) + norm_backward(mid_stream, grad_normed)).astype(bf16)
    grad_context = jnp.dot(grad_mid, output_weight[top], preferred_element_type=f32).astype(bf16)
    grad_qkv = attend_backward(probs, queries, key_rows, values, grad_context)
    partial = contract_cols(grad_qkv, triple[top]).astype(bf16).reshape(n, share, width)
    quarters = jnp.stack([final_part[:, k * quarter : (k + 1) * quarter] for k in range(4)])
    sent = jnp.concatenate([partial, jnp.tile(quarters, (4, 1, 1))], axis=2)
    came = lax.all_to_all(sent, MP, 0, 0, tiled=True)
    own = jnp.sum(came[:, :, :width].astype(f32), axis=0).astype(bf16)
    column = came[:, :, width:].reshape(rows, quarter)
    wide1 = [
        contract_rows(normed_mid, grad_preact),
        contract_rows(upstream, activated),
        contract_rows(normed, grad_qkv),
        contract_rows(grad_mid, context),
    ]
    sums1, sent1 = y_stage(wide1, y_turns)
    grad_input = all_rows(after(own, *sent1), MP)
    upstream = (grad_mid.astype(f32) + norm_backward(stream, grad_input)).astype(bf16)
    (normed, stream, queries, key_rows, values, probs, context,
     mid_stream, normed_mid, preact, activated) = saved[0]
    grad_act = jnp.dot(upstream, downward_weight[0], preferred_element_type=f32).astype(bf16)
    _, gate_back = jax.vjp(smooth_gate, preact)
    grad_preact = gate_back(grad_act.astype(f32))[0].astype(bf16)
    partial = contract_cols(grad_preact, upward_weight[0]).astype(bf16)
    own = share_rows(partial, MP).astype(bf16)
    wide0 = [contract_rows(normed_mid, grad_preact), contract_rows(upstream, activated)]
    sums0, sent0 = y_stage(wide0, y_turns)
    grad_normed = all_rows(after(own, *sent0), MP)
    grad_mid = (upstream.astype(f32) + norm_backward(mid_stream, grad_normed)).astype(bf16)
    grad_context = jnp.dot(grad_mid, output_weight[0], preferred_element_type=f32).astype(bf16)
    grad_qkv = attend_backward(probs, queries, key_rows, values, grad_context)
    late = [contract_rows(normed, grad_qkv), contract_rows(grad_mid, context)]
    late = jnp.concatenate([g.astype(bf16) for g in late], axis=1)
    column = after(column, late)
    columns = [column] + [moved(column, "x", step) for step in range(1, 4)]
    sums1 = total(sums1).astype(bf16)
    sums0 = total(sums0).astype(bf16)
    sums = jnp.concatenate([sums1, sums0], axis=3)
    sums = quad_stage(sums.reshape(4, *sums.shape[2:]), quad_turns)
    late = share_rows(late, DP)
    final_stream = jnp.concatenate(
        [lax.select_n(x_slots[k].astype(jnp.int32), *columns) for k in range(4)], axis=1
    )
    sums = total(sums)

    def cut(x, first, size):
        return x[:, first : first + size]

    ff = upward_weight.shape[-1]
    first0 = 2 * ff + 4 * heads
    return (
        final_stream,
        jnp.stack([
            cut(late, 0, 3 * heads).reshape(-1, 3, heads),
            cut(sums, 2 * ff, 3 * heads).reshape(-1, 3, heads),
        ]),
        jnp.stack([cut(late, 3 * heads, heads), cut(sums, 2 * ff + 3 * heads, heads)]),
        jnp.stack([cut(sums, first0, ff), cut(sums, 0, ff)]),
        jnp.stack([cut(sums, first0 + ff, ff), cut(sums, ff, ff)]),
    )


def solution(mesh):
    torus = Mesh(mesh.devices.reshape(2, 4, 2, 4, 4), (*DP, *MP))
    placed = (
        P(DP, None),
        P(DP),
        P(DP, None),
        P(None, None, None, MP),
        P(None, None, MP),
        P(None, None, MP),
        P(None, None, MP),
    )
    return jax.shard_map(
        step,
        mesh=torus,
        in_specs=placed,
        out_specs=(
            P(DP, None),
            P(None, DP, None, MP),
            P(None, DP, MP),
            P(None, DP, MP),
            P(None, DP, MP),
        ),
        check_vma=False,
    )
```

```python
import jax
import jax.numpy as jnp
from jax import lax
from jax.sharding import Mesh
from jax.sharding import PartitionSpec as P


HD = 64
SLATE = 256
LAYERS = 2
DP = ("z_lo", "y", "core")
MP = ("z_hi", "x")


epsilon = 1e-06
bf16 = jnp.bfloat16
f32 = jnp.float32


def share_rows(x, axis):
    n = lax.axis_size(axis)
    blocks = x.reshape(n, x.shape[0] // n, x.shape[1])
    blocks = lax.all_to_all(blocks, axis, 0, 0, tiled=True)
    return jnp.sum(blocks.astype(f32), axis=0)


def all_rows(x, axis):
    n = lax.axis_size(axis)
    copies = jnp.broadcast_to(x[None], (n, *x.shape))
    blocks = lax.all_to_all(copies, axis, 0, 0, tiled=True)
    return blocks.reshape(n * x.shape[0], x.shape[1])


def after(x, *others):
    return lax.optimization_barrier((x, *others))[0]


def moved(x, axis, step):
    n = lax.axis_size(axis)
    return lax.ppermute(x, axis, [(k, (k + step) % n) for k in range(n)])


def pick(x, index):
    return lax.dynamic_index_in_dim(x, index, 0, keepdims=False)


def total(parts):
    return sum(p.astype(f32) for p in parts)


def y_stage(grads):
    joined = jnp.concatenate([g.astype(bf16) for g in grads], axis=1)
    rows, cols = joined.shape
    parts = jnp.moveaxis(joined.reshape(2, 4, 2, rows // 16, cols), 1, 0)
    here = lax.axis_index("y")
    sent = [pick(parts, (here + k) % 4) for k in range(1, 4)]
    return [pick(parts, here)] + [moved(s, "y", k) for k, s in enumerate(sent, 1)], sent


def quad_stage(parts):
    axes = ("z_lo", "core")
    here = lax.axis_index(axes)
    return [pick(parts, here)] + [
        lax.ppermute(pick(parts, here ^ k), axes, [(i, i ^ k) for i in range(4)]) for k in range(1, 4)
    ]


def normalize(stream):
    widened = stream.astype(f32)
    rscale = lax.rsqrt(jnp.mean(widened * widened, axis=-1, keepdims=True) + epsilon)
    scaled = widened * rscale
    return (scaled.astype(bf16), scaled, rscale)


def norm_backward(scaled, rscale, upward):
    inner = jnp.mean(upward * scaled, axis=-1, keepdims=True)
    return rscale * (upward - scaled * inner)


def smooth_gate(preact):
    return jax.nn.gelu(preact, approximate=True)


def dot(left, right, dims):
    return lax.dot_general(left, right, (dims, ((), ())), preferred_element_type=f32)


def contract_rows(left, right):
    return dot(left, right, ((0,), (0,)))


def contract_cols(left, right):
    return dot(left, right, ((1,), (1,)))


def attend(queries, key_rows, values, live):
    scores = contract_cols(queries, key_rows) * HD ** (-0.5)
    weights = jnp.exp(scores) * live
    probs = weights / jnp.sum(weights, axis=-1, keepdims=True)
    context = jnp.dot(probs.astype(bf16), values, preferred_element_type=f32).astype(bf16)
    return probs, context


def attend_backward(probs, queries, key_rows, values, grad_context):
    grad_prob = contract_cols(grad_context, values)
    grad_value = contract_rows(probs.astype(bf16), grad_context).astype(bf16)
    inner = jnp.sum(grad_prob * probs, axis=-1, keepdims=True)
    grad_score = (probs * (grad_prob - inner) * HD ** (-0.5)).astype(bf16)
    grad_query = jnp.dot(grad_score, key_rows, preferred_element_type=f32).astype(bf16)
    grad_key = contract_rows(grad_score, queries).astype(bf16)
    return jnp.concatenate([grad_query, grad_key, grad_value], axis=1)


def step(tokens, lengths, cotangent, triple_weight, output_weight, upward_weight, downward_weight):
    rows, width = tokens.shape
    n = lax.axis_size(MP)
    share = rows // n
    start = lax.axis_index(MP) * share

    def part(x):
        return lax.dynamic_slice_in_dim(x, start, share, 0)

    live = (jnp.arange(SLATE)[None, :] < lengths[:, None]).astype(f32)
    triple = [triple_weight[l].reshape(width, -1) for l in range(LAYERS)]
    saved = []
    stream = tokens
    stream_part = part(tokens)
    for l in range(LAYERS):
        normed, scaled, rscale = normalize(stream)
        qkv = jnp.dot(normed, triple[l], preferred_element_type=f32).astype(bf16)
        queries, key_rows, values = (qkv[:, k * HD : (k + 1) * HD] for k in range(3))
        probs, context = attend(queries, key_rows, values, live)
        partial_att = contract_cols(context, output_weight[l]).astype(bf16)
        mid_part = (stream_part.astype(f32) + share_rows(partial_att, MP)).astype(bf16)
        mid_stream = all_rows(mid_part, MP)
        normed_mid, scaled_mid, rscale_mid = normalize(mid_stream)
        preact = jnp.dot(normed_mid, upward_weight[l], preferred_element_type=f32)
        activated = smooth_gate(preact).astype(bf16)
        partial_ffn = contract_cols(activated, downward_weight[l]).astype(bf16)
        saved.append((normed, scaled, rscale, queries, key_rows, values, probs, context,
                      scaled_mid, rscale_mid, normed_mid, preact, activated))
        if l + 1 < LAYERS:
            stream_part = (mid_part.astype(f32) + share_rows(partial_ffn, MP)).astype(bf16)
            stream = all_rows(stream_part, MP)

    top = LAYERS - 1
    quarter = width // 4
    heads = triple_weight.shape[-1]
    x_here = lax.axis_index("x")

    (normed, scaled, rscale, queries, key_rows, values, probs, context,
     scaled_mid, rscale_mid, normed_mid, preact, activated) = saved[top]
    upstream = cotangent
    grad_act = jnp.dot(upstream, downward_weight[top], preferred_element_type=f32).astype(bf16)
    _, gate_back = jax.vjp(smooth_gate, preact)
    grad_preact = gate_back(grad_act.astype(f32))[0].astype(bf16)
    partial = contract_cols(grad_preact, upward_weight[top]).astype(bf16)
    shares = jnp.stack([partial_ffn[:, k * quarter : (k + 1) * quarter] for k in range(4)])
    shares = [pick(shares, x_here)] + [
        moved(pick(shares, (x_here + k) % 4), "x", k) for k in range(1, 4)
    ]
    own = share_rows(partial, MP).astype(bf16)
    shares = total(shares).astype(bf16).reshape(n, share, quarter)
    sent = jnp.concatenate([jnp.broadcast_to(own[None], (n, share, width)), shares], axis=2)
    came = lax.all_to_all(after(sent, rscale_mid), MP, 0, 0, tiled=True)
    grad_normed = came[:, :, :width].reshape(rows, width).astype(f32)
    ffn_part = jnp.sum(came[:, :, width:].reshape(4, 4, share, quarter).astype(f32), axis=0)
    ffn_part = jnp.concatenate([ffn_part[k] for k in range(4)], axis=1)
    final_part = (mid_part.astype(f32) + ffn_part).astype(bf16)
    grad_mid = (upstream.astype(f32) + norm_backward(scaled_mid, rscale_mid, grad_normed)).astype(bf16)
    grad_context = jnp.dot(grad_mid, output_weight[top], preferred_element_type=f32).astype(bf16)
    grad_qkv = attend_backward(probs, queries, key_rows, values, grad_context)
    partial = contract_cols(grad_qkv, triple[top]).astype(bf16).reshape(n, share, width)
    quarters = jnp.stack([final_part[:, k * quarter : (k + 1) * quarter] for k in range(4)])
    sent = jnp.concatenate([partial, jnp.tile(quarters, (4, 1, 1))], axis=2)
    came = lax.all_to_all(sent, MP, 0, 0, tiled=True)
    own = jnp.sum(came[:, :, :width].astype(f32), axis=0).astype(bf16)
    column = came[:, :, width:].reshape(rows, quarter)
    wide1 = [
        contract_rows(normed_mid, grad_preact),
        contract_rows(upstream, activated),
        contract_rows(normed, grad_qkv),
        contract_rows(grad_mid, context),
    ]
    sums1, sent1 = y_stage(wide1)
    grad_input = all_rows(after(own, rscale, *sent1), MP).astype(f32)
    upstream = (grad_mid.astype(f32) + norm_backward(scaled, rscale, grad_input)).astype(bf16)
    (normed, scaled, rscale, queries, key_rows, values, probs, context,
     scaled_mid, rscale_mid, normed_mid, preact, activated) = saved[0]
    grad_act = jnp.dot(upstream, downward_weight[0], preferred_element_type=f32).astype(bf16)
    _, gate_back = jax.vjp(smooth_gate, preact)
    grad_preact = gate_back(grad_act.astype(f32))[0].astype(bf16)
    partial = contract_cols(grad_preact, upward_weight[0]).astype(bf16)
    own = share_rows(partial, MP).astype(bf16)
    wide0 = [contract_rows(normed_mid, grad_preact), contract_rows(upstream, activated)]
    sums0, sent0 = y_stage(wide0)
    grad_normed = all_rows(after(own, rscale_mid, *sent0), MP).astype(f32)
    grad_mid = (upstream.astype(f32) + norm_backward(scaled_mid, rscale_mid, grad_normed)).astype(bf16)
    grad_context = jnp.dot(grad_mid, output_weight[0], preferred_element_type=f32).astype(bf16)
    grad_qkv = attend_backward(probs, queries, key_rows, values, grad_context)
    late = [contract_rows(normed, grad_qkv), contract_rows(grad_mid, context)]
    late = jnp.concatenate([g.astype(bf16) for g in late], axis=1)
    column = after(column, late)
    columns = [column] + [moved(column, "x", step) for step in range(1, 4)]
    sums1 = total(sums1).astype(bf16)
    sums0 = total(sums0).astype(bf16)
    sums = jnp.concatenate([sums1, sums0], axis=3)
    sums = quad_stage(sums.reshape(4, *sums.shape[2:]))
    late = share_rows(late, DP)
    final_stream = jnp.concatenate(
        [lax.select_n((x_here - k) % 4, *columns) for k in range(4)], axis=1
    )
    sums = total(sums)

    def cut(x, first, size):
        return x[:, first : first + size]

    ff = upward_weight.shape[-1]
    first0 = 2 * ff + 4 * heads
    return (
        final_stream,
        jnp.stack([
            cut(late, 0, 3 * heads).reshape(-1, 3, heads),
            cut(sums, 2 * ff, 3 * heads).reshape(-1, 3, heads),
        ]),
        jnp.stack([cut(late, 3 * heads, heads), cut(sums, 2 * ff + 3 * heads, heads)]),
        jnp.stack([cut(sums, first0, ff), cut(sums, 0, ff)]),
        jnp.stack([cut(sums, first0 + ff, ff), cut(sums, ff, ff)]),
    )


def solution(mesh):
    torus = Mesh(mesh.devices.reshape(2, 4, 2, 4, 4), (*DP, *MP))
    placed = (
        P(DP, None),
        P(DP),
        P(DP, None),
        P(None, None, None, MP),
        P(None, None, MP),
        P(None, None, MP),
        P(None, None, MP),
    )
    return jax.shard_map(
        step,
        mesh=torus,
        in_specs=placed,
        out_specs=(
            P(DP, None),
            P(None, DP, None, MP),
            P(None, DP, MP),
            P(None, DP, MP),
            P(None, DP, MP),
        ),
        check_vma=False,
    )
```

```python
import jax
import jax.numpy as jnp
from jax import lax
from jax.sharding import Mesh
from jax.sharding import PartitionSpec as P


HD = 64
SLATE = 256
LAYERS = 2
DP = ("z_lo", "y", "core")
MP = ("z_hi", "x")


STAGGER = 416

epsilon = 1e-06
bf16 = jnp.bfloat16
f32 = jnp.float32


def share_rows(x, axis):
    n = lax.axis_size(axis)
    blocks = x.reshape(n, x.shape[0] // n, x.shape[1])
    blocks = lax.all_to_all(blocks, axis, 0, 0, tiled=True)
    return jnp.sum(blocks.astype(f32), axis=0)


def all_rows(x, axis):
    n = lax.axis_size(axis)
    copies = jnp.broadcast_to(x[None], (n, *x.shape))
    blocks = lax.all_to_all(copies, axis, 0, 0, tiled=True)
    return blocks.reshape(n * x.shape[0], x.shape[1])


def after(x, *others):
    return lax.optimization_barrier((x, *others))[0]


def moved(x, axis, step):
    n = lax.axis_size(axis)
    return lax.ppermute(x, axis, [(k, (k + step) % n) for k in range(n)])


def pick(x, index):
    return lax.dynamic_index_in_dim(x, index, 0, keepdims=False)


def total(parts):
    return sum(p.astype(f32) for p in parts)


def y_stage(grads):
    joined = jnp.concatenate([g.astype(bf16) for g in grads], axis=1)
    rows, cols = joined.shape
    parts = jnp.moveaxis(joined.reshape(2, 4, 2, rows // 16, cols), 1, 0)
    here = lax.axis_index("y")
    sent = [pick(parts, (here + k) % 4) for k in range(1, 4)]
    return [pick(parts, here)] + [moved(s, "y", k) for k, s in enumerate(sent, 1)], sent


def quad_stage(parts):
    axes = ("z_lo", "core")
    here = lax.axis_index(axes)
    return [pick(parts, here)] + [
        lax.ppermute(pick(parts, here ^ k), axes, [(i, i ^ k) for i in range(4)]) for k in range(1, 4)
    ]


def later_start(tokens):
    steps = lax.axis_index("core") * STAGGER
    return lax.fori_loop(0, steps, lambda _, v: jnp.tanh(v) * 1.5, tokens[:8, :128].astype(f32))


def normalize(stream):
    widened = stream.astype(f32)
    rscale = lax.rsqrt(jnp.mean(widened * widened, axis=-1, keepdims=True) + epsilon)
    scaled = widened * rscale
    return (scaled.astype(bf16), scaled, rscale)


def norm_backward(scaled, rscale, upward):
    inner = jnp.mean(upward * scaled, axis=-1, keepdims=True)
    return rscale * (upward - scaled * inner)


def smooth_gate(preact):
    return jax.nn.gelu(preact, approximate=True)


def dot(left, right, dims):
    return lax.dot_general(left, right, (dims, ((), ())), preferred_element_type=f32)


def contract_rows(left, right):
    return dot(left, right, ((0,), (0,)))


def contract_cols(left, right):
    return dot(left, right, ((1,), (1,)))


def attend(queries, key_rows, values, live):
    scores = contract_cols(queries, key_rows) * HD ** (-0.5)
    weights = jnp.exp(scores) * live
    probs = weights / jnp.sum(weights, axis=-1, keepdims=True)
    context = jnp.dot(probs.astype(bf16), values, preferred_element_type=f32).astype(bf16)
    return probs, context


def attend_backward(probs, queries, key_rows, values, grad_context):
    grad_prob = contract_cols(grad_context, values)
    grad_value = contract_rows(probs.astype(bf16), grad_context).astype(bf16)
    inner = jnp.sum(grad_prob * probs, axis=-1, keepdims=True)
    grad_score = (probs * (grad_prob - inner) * HD ** (-0.5)).astype(bf16)
    grad_query = jnp.dot(grad_score, key_rows, preferred_element_type=f32).astype(bf16)
    grad_key = contract_rows(grad_score, queries).astype(bf16)
    return jnp.concatenate([grad_query, grad_key, grad_value], axis=1)


def step(tokens, lengths, cotangent, triple_weight, output_weight, upward_weight, downward_weight):
    rows, width = tokens.shape
    n = lax.axis_size(MP)
    share = rows // n
    start = lax.axis_index(MP) * share

    def part(x):
        return lax.dynamic_slice_in_dim(x, start, share, 0)

    live = (jnp.arange(SLATE)[None, :] < lengths[:, None]).astype(f32)
    triple = [triple_weight[l].reshape(width, -1) for l in range(LAYERS)]
    saved = []
    stream = tokens
    stream_part = part(tokens)
    for l in range(LAYERS):
        normed, scaled, rscale = normalize(stream)
        qkv = jnp.dot(normed, triple[l], preferred_element_type=f32).astype(bf16)
        queries, key_rows, values = (qkv[:, k * HD : (k + 1) * HD] for k in range(3))
        probs, context = attend(queries, key_rows, values, live)
        partial_att = contract_cols(context, output_weight[l]).astype(bf16)
        if l == 0:
            partial_att = after(partial_att, later_start(tokens))
        mid_part = (stream_part.astype(f32) + share_rows(partial_att, MP)).astype(bf16)
        mid_stream = all_rows(mid_part, MP)
        normed_mid, scaled_mid, rscale_mid = normalize(mid_stream)
        preact = jnp.dot(normed_mid, upward_weight[l], preferred_element_type=f32)
        activated = smooth_gate(preact).astype(bf16)
        partial_ffn = contract_cols(activated, downward_weight[l]).astype(bf16)
        saved.append((normed, scaled, rscale, queries, key_rows, values, probs, context,
                      scaled_mid, rscale_mid, normed_mid, preact, activated))
        if l + 1 < LAYERS:
            stream_part = (mid_part.astype(f32) + share_rows(partial_ffn, MP)).astype(bf16)
            stream = all_rows(stream_part, MP)

    top = LAYERS - 1
    quarter = width // 4
    heads = triple_weight.shape[-1]
    x_here = lax.axis_index("x")

    (normed, scaled, rscale, queries, key_rows, values, probs, context,
     scaled_mid, rscale_mid, normed_mid, preact, activated) = saved[top]
    upstream = cotangent
    grad_act = jnp.dot(upstream, downward_weight[top], preferred_element_type=f32).astype(bf16)
    _, gate_back = jax.vjp(smooth_gate, preact)
    grad_preact = gate_back(grad_act.astype(f32))[0].astype(bf16)
    partial = contract_cols(grad_preact, upward_weight[top]).astype(bf16)
    shares = jnp.stack([partial_ffn[:, k * quarter : (k + 1) * quarter] for k in range(4)])
    shares = [pick(shares, x_here)] + [
        moved(pick(shares, (x_here + k) % 4), "x", k) for k in range(1, 4)
    ]
    own = share_rows(partial, MP).astype(bf16)
    shares = total(shares).astype(bf16).reshape(n, share, quarter)
    sent = jnp.concatenate([jnp.broadcast_to(own[None], (n, share, width)), shares], axis=2)
    came = lax.all_to_all(after(sent, rscale_mid), MP, 0, 0, tiled=True)
    grad_normed = came[:, :, :width].reshape(rows, width).astype(f32)
    ffn_part = jnp.sum(came[:, :, width:].reshape(4, 4, share, quarter).astype(f32), axis=0)
    ffn_part = jnp.concatenate([ffn_part[k] for k in range(4)], axis=1)
    final_part = (mid_part.astype(f32) + ffn_part).astype(bf16)
    grad_mid = (upstream.astype(f32) + norm_backward(scaled_mid, rscale_mid, grad_normed)).astype(bf16)
    grad_context = jnp.dot(grad_mid, output_weight[top], preferred_element_type=f32).astype(bf16)
    grad_qkv = attend_backward(probs, queries, key_rows, values, grad_context)
    partial = contract_cols(grad_qkv, triple[top]).astype(bf16).reshape(n, share, width)
    quarters = jnp.stack([final_part[:, k * quarter : (k + 1) * quarter] for k in range(4)])
    sent = jnp.concatenate([partial, jnp.tile(quarters, (4, 1, 1))], axis=2)
    came = lax.all_to_all(sent, MP, 0, 0, tiled=True)
    own = jnp.sum(came[:, :, :width].astype(f32), axis=0).astype(bf16)
    column = came[:, :, width:].reshape(rows, quarter)
    wide1 = [
        contract_rows(normed_mid, grad_preact),
        contract_rows(upstream, activated),
        contract_rows(normed, grad_qkv),
        contract_rows(grad_mid, context),
    ]
    sums1, sent1 = y_stage(wide1)
    grad_input = all_rows(after(own, rscale, *sent1), MP).astype(f32)
    upstream = (grad_mid.astype(f32) + norm_backward(scaled, rscale, grad_input)).astype(bf16)
    (normed, scaled, rscale, queries, key_rows, values, probs, context,
     scaled_mid, rscale_mid, normed_mid, preact, activated) = saved[0]
    grad_act = jnp.dot(upstream, downward_weight[0], preferred_element_type=f32).astype(bf16)
    _, gate_back = jax.vjp(smooth_gate, preact)
    grad_preact = gate_back(grad_act.astype(f32))[0].astype(bf16)
    partial = contract_cols(grad_preact, upward_weight[0]).astype(bf16)
    own = share_rows(partial, MP).astype(bf16)
    wide0 = [contract_rows(normed_mid, grad_preact), contract_rows(upstream, activated)]
    sums0, sent0 = y_stage(wide0)
    grad_normed = all_rows(after(own, rscale_mid, *sent0), MP).astype(f32)
    grad_mid = (upstream.astype(f32) + norm_backward(scaled_mid, rscale_mid, grad_normed)).astype(bf16)
    grad_context = jnp.dot(grad_mid, output_weight[0], preferred_element_type=f32).astype(bf16)
    grad_qkv = attend_backward(probs, queries, key_rows, values, grad_context)
    late = [contract_rows(normed, grad_qkv), contract_rows(grad_mid, context)]
    late = jnp.concatenate([g.astype(bf16) for g in late], axis=1)
    column = after(column, late)
    columns = [column] + [moved(column, "x", step) for step in range(1, 4)]
    sums1 = total(sums1).astype(bf16)
    sums0 = total(sums0).astype(bf16)
    sums = jnp.concatenate([sums1, sums0], axis=3)
    sums = quad_stage(sums.reshape(4, *sums.shape[2:]))
    late = share_rows(late, DP)
    final_stream = jnp.concatenate(
        [lax.select_n((x_here - k) % 4, *columns) for k in range(4)], axis=1
    )
    sums = total(sums)

    def cut(x, first, size):
        return x[:, first : first + size]

    ff = upward_weight.shape[-1]
    first0 = 2 * ff + 4 * heads
    return (
        final_stream,
        jnp.stack([
            cut(late, 0, 3 * heads).reshape(-1, 3, heads),
            cut(sums, 2 * ff, 3 * heads).reshape(-1, 3, heads),
        ]),
        jnp.stack([cut(late, 3 * heads, heads), cut(sums, 2 * ff + 3 * heads, heads)]),
        jnp.stack([cut(sums, first0, ff), cut(sums, 0, ff)]),
        jnp.stack([cut(sums, first0 + ff, ff), cut(sums, ff, ff)]),
    )


def solution(mesh):
    torus = Mesh(mesh.devices.reshape(2, 4, 2, 4, 4), (*DP, *MP))
    placed = (
        P(DP, None),
        P(DP),
        P(DP, None),
        P(None, None, None, MP),
        P(None, None, MP),
        P(None, None, MP),
        P(None, None, MP),
    )
    return jax.shard_map(
        step,
        mesh=torus,
        in_specs=placed,
        out_specs=(
            P(DP, None),
            P(None, DP, None, MP),
            P(None, DP, MP),
            P(None, DP, MP),
            P(None, DP, MP),
        ),
        check_vma=False,
    )
```

```python
import jax
import jax.numpy as jnp
from jax import lax
from jax.sharding import Mesh
from jax.sharding import PartitionSpec as P


HD = 64
SLATE = 256
LAYERS = 2
DP = ("z_lo", "y", "core")
MP = ("z_hi", "x")


STAGGER = 520

epsilon = 1e-06
bf16 = jnp.bfloat16
f32 = jnp.float32


def share_rows(x, axis):
    n = lax.axis_size(axis)
    blocks = x.reshape(n, x.shape[0] // n, x.shape[1])
    blocks = lax.all_to_all(blocks, axis, 0, 0, tiled=True)
    return jnp.sum(blocks.astype(f32), axis=0)


def all_rows(x, axis):
    n = lax.axis_size(axis)
    copies = jnp.broadcast_to(x[None], (n, *x.shape))
    blocks = lax.all_to_all(copies, axis, 0, 0, tiled=True)
    return blocks.reshape(n * x.shape[0], x.shape[1])


def after(x, *others):
    return lax.optimization_barrier((x, *others))[0]


def moved(x, axis, step):
    n = lax.axis_size(axis)
    return lax.ppermute(x, axis, [(k, (k + step) % n) for k in range(n)])


def pick(x, index):
    return lax.dynamic_index_in_dim(x, index, 0, keepdims=False)


def total(parts):
    return sum(p.astype(f32) for p in parts)


def y_stage(grads):
    joined = jnp.concatenate([g.astype(bf16) for g in grads], axis=1)
    rows, cols = joined.shape
    parts = jnp.moveaxis(joined.reshape(2, 4, 2, rows // 16, cols), 1, 0)
    here = lax.axis_index("y")
    sent = [pick(parts, (here + k) % 4) for k in range(1, 4)]
    return [pick(parts, here)] + [moved(s, "y", k) for k, s in enumerate(sent, 1)], sent


def quad_stage(parts):
    axes = ("z_lo", "core")
    here = lax.axis_index(axes)
    return [pick(parts, here)] + [
        lax.ppermute(pick(parts, here ^ k), axes, [(i, i ^ k) for i in range(4)]) for k in range(1, 4)
    ]


def later_start(tokens):
    steps = lax.axis_index("core") * STAGGER
    state = lax.fori_loop(0, steps, lambda _, v: jnp.tanh(v) * 1.5, tokens[:8, :128].astype(f32) * 0.25)
    return (state[0, 0] > 4.0).astype(jnp.int32)


def normalize(stream):
    widened = stream.astype(f32)
    rscale = lax.rsqrt(jnp.mean(widened * widened, axis=-1, keepdims=True) + epsilon)
    scaled = widened * rscale
    return (scaled.astype(bf16), scaled, rscale)


def norm_backward(scaled, rscale, upward):
    inner = jnp.mean(upward * scaled, axis=-1, keepdims=True)
    return rscale * (upward - scaled * inner)


def smooth_gate(preact):
    return jax.nn.gelu(preact, approximate=True)


def dot(left, right, dims):
    return lax.dot_general(left, right, (dims, ((), ())), preferred_element_type=f32)


def contract_rows(left, right):
    return dot(left, right, ((0,), (0,)))


def contract_cols(left, right):
    return dot(left, right, ((1,), (1,)))


def attend(queries, key_rows, values, live):
    scores = contract_cols(queries, key_rows) * HD ** (-0.5)
    weights = jnp.exp(scores) * live
    probs = weights / jnp.sum(weights, axis=-1, keepdims=True)
    context = jnp.dot(probs.astype(bf16), values, preferred_element_type=f32).astype(bf16)
    return probs, context


def attend_backward(probs, queries, key_rows, values, grad_context):
    grad_prob = contract_cols(grad_context, values)
    grad_value = contract_rows(probs.astype(bf16), grad_context).astype(bf16)
    inner = jnp.sum(grad_prob * probs, axis=-1, keepdims=True)
    grad_score = (probs * (grad_prob - inner) * HD ** (-0.5)).astype(bf16)
    grad_query = jnp.dot(grad_score, key_rows, preferred_element_type=f32).astype(bf16)
    grad_key = contract_rows(grad_score, queries).astype(bf16)
    return jnp.concatenate([grad_query, grad_key, grad_value], axis=1)


def step(tokens, lengths, cotangent, triple_weight, output_weight, upward_weight, downward_weight):
    rows, width = tokens.shape
    n = lax.axis_size(MP)
    share = rows // n
    start = lax.axis_index(MP) * share

    def part(x):
        return lax.dynamic_slice_in_dim(x, start, share, 0)

    lengths = lengths + later_start(tokens)
    live = (jnp.arange(SLATE)[None, :] < lengths[:, None]).astype(f32)
    triple = [triple_weight[l].reshape(width, -1) for l in range(LAYERS)]
    saved = []
    stream = tokens
    stream_part = part(tokens)
    for l in range(LAYERS):
        normed, scaled, rscale = normalize(stream)
        qkv = jnp.dot(normed, triple[l], preferred_element_type=f32).astype(bf16)
        queries, key_rows, values = (qkv[:, k * HD : (k + 1) * HD] for k in range(3))
        probs, context = attend(queries, key_rows, values, live)
        partial_att = contract_cols(context, output_weight[l]).astype(bf16)
        mid_part = (stream_part.astype(f32) + share_rows(partial_att, MP)).astype(bf16)
        mid_stream = all_rows(mid_part, MP)
        normed_mid, scaled_mid, rscale_mid = normalize(mid_stream)
        preact = jnp.dot(normed_mid, upward_weight[l], preferred_element_type=f32)
        activated = smooth_gate(preact).astype(bf16)
        partial_ffn = contract_cols(activated, downward_weight[l]).astype(bf16)
        saved.append((normed, scaled, rscale, queries, key_rows, values, probs, context,
                      scaled_mid, rscale_mid, normed_mid, preact, activated))
        if l + 1 < LAYERS:
            stream_part = (mid_part.astype(f32) + share_rows(partial_ffn, MP)).astype(bf16)
            stream = all_rows(stream_part, MP)

    top = LAYERS - 1
    quarter = width // 4
    heads = triple_weight.shape[-1]
    x_here = lax.axis_index("x")

    (normed, scaled, rscale, queries, key_rows, values, probs, context,
     scaled_mid, rscale_mid, normed_mid, preact, activated) = saved[top]
    upstream = cotangent
    grad_act = jnp.dot(upstream, downward_weight[top], preferred_element_type=f32).astype(bf16)
    _, gate_back = jax.vjp(smooth_gate, preact)
    grad_preact = gate_back(grad_act.astype(f32))[0].astype(bf16)
    partial = contract_cols(grad_preact, upward_weight[top]).astype(bf16)
    shares = jnp.stack([partial_ffn[:, k * quarter : (k + 1) * quarter] for k in range(4)])
    shares = [pick(shares, x_here)] + [
        moved(pick(shares, (x_here + k) % 4), "x", k) for k in range(1, 4)
    ]
    own = share_rows(partial, MP).astype(bf16)
    shares = total(shares).astype(bf16).reshape(n, share, quarter)
    sent = jnp.concatenate([jnp.broadcast_to(own[None], (n, share, width)), shares], axis=2)
    came = lax.all_to_all(after(sent, rscale_mid), MP, 0, 0, tiled=True)
    grad_normed = came[:, :, :width].reshape(rows, width).astype(f32)
    ffn_part = jnp.sum(came[:, :, width:].reshape(4, 4, share, quarter).astype(f32), axis=0)
    ffn_part = jnp.concatenate([ffn_part[k] for k in range(4)], axis=1)
    final_part = (mid_part.astype(f32) + ffn_part).astype(bf16)
    grad_mid = (upstream.astype(f32) + norm_backward(scaled_mid, rscale_mid, grad_normed)).astype(bf16)
    grad_context = jnp.dot(grad_mid, output_weight[top], preferred_element_type=f32).astype(bf16)
    grad_qkv = attend_backward(probs, queries, key_rows, values, grad_context)
    partial = contract_cols(grad_qkv, triple[top]).astype(bf16).reshape(n, share, width)
    quarters = jnp.stack([final_part[:, k * quarter : (k + 1) * quarter] for k in range(4)])
    sent = jnp.concatenate([partial, jnp.tile(quarters, (4, 1, 1))], axis=2)
    came = lax.all_to_all(sent, MP, 0, 0, tiled=True)
    own = jnp.sum(came[:, :, :width].astype(f32), axis=0).astype(bf16)
    column = came[:, :, width:].reshape(rows, quarter)
    wide1 = [
        contract_rows(normed_mid, grad_preact),
        contract_rows(upstream, activated),
        contract_rows(normed, grad_qkv),
        contract_rows(grad_mid, context),
    ]
    sums1, sent1 = y_stage(wide1)
    grad_input = all_rows(after(own, rscale, *sent1), MP).astype(f32)
    upstream = (grad_mid.astype(f32) + norm_backward(scaled, rscale, grad_input)).astype(bf16)
    (normed, scaled, rscale, queries, key_rows, values, probs, context,
     scaled_mid, rscale_mid, normed_mid, preact, activated) = saved[0]
    grad_act = jnp.dot(upstream, downward_weight[0], preferred_element_type=f32).astype(bf16)
    _, gate_back = jax.vjp(smooth_gate, preact)
    grad_preact = gate_back(grad_act.astype(f32))[0].astype(bf16)
    partial = contract_cols(grad_preact, upward_weight[0]).astype(bf16)
    own = share_rows(partial, MP).astype(bf16)
    wide0 = [contract_rows(normed_mid, grad_preact), contract_rows(upstream, activated)]
    sums0, sent0 = y_stage(wide0)
    grad_normed = all_rows(after(own, rscale_mid, *sent0), MP).astype(f32)
    grad_mid = (upstream.astype(f32) + norm_backward(scaled_mid, rscale_mid, grad_normed)).astype(bf16)
    grad_context = jnp.dot(grad_mid, output_weight[0], preferred_element_type=f32).astype(bf16)
    grad_qkv = attend_backward(probs, queries, key_rows, values, grad_context)
    late = [contract_rows(normed, grad_qkv), contract_rows(grad_mid, context)]
    late = jnp.concatenate([g.astype(bf16) for g in late], axis=1)
    column = after(column, late)
    columns = [column] + [moved(column, "x", step) for step in range(1, 4)]
    sums1 = total(sums1).astype(bf16)
    sums0 = total(sums0).astype(bf16)
    sums = jnp.concatenate([sums1, sums0], axis=3)
    sums = quad_stage(sums.reshape(4, *sums.shape[2:]))
    late = share_rows(late, DP)
    final_stream = jnp.concatenate(
        [lax.select_n((x_here - k) % 4, *columns) for k in range(4)], axis=1
    )
    sums = total(sums)

    def cut(x, first, size):
        return x[:, first : first + size]

    ff = upward_weight.shape[-1]
    first0 = 2 * ff + 4 * heads
    return (
        final_stream,
        jnp.stack([
            cut(late, 0, 3 * heads).reshape(-1, 3, heads),
            cut(sums, 2 * ff, 3 * heads).reshape(-1, 3, heads),
        ]),
        jnp.stack([cut(late, 3 * heads, heads), cut(sums, 2 * ff + 3 * heads, heads)]),
        jnp.stack([cut(sums, first0, ff), cut(sums, 0, ff)]),
        jnp.stack([cut(sums, first0 + ff, ff), cut(sums, ff, ff)]),
    )


def solution(mesh):
    torus = Mesh(mesh.devices.reshape(2, 4, 2, 4, 4), (*DP, *MP))
    placed = (
        P(DP, None),
        P(DP),
        P(DP, None),
        P(None, None, None, MP),
        P(None, None, MP),
        P(None, None, MP),
        P(None, None, MP),
    )
    return jax.shard_map(
        step,
        mesh=torus,
        in_specs=placed,
        out_specs=(
            P(DP, None),
            P(None, DP, None, MP),
            P(None, DP, MP),
            P(None, DP, MP),
            P(None, DP, MP),
        ),
        check_vma=False,
    )
```
